32 devices in a mesh: groups: 2 (over y), section: 2 (over x), expert: 4 (over z), pair: 2 (over core).
Axes of the slice: x: 2, y: 2, z: 4, core: 2. Of those that a mesh axis runs over, the one named last changes fastest.
Arguments:
- transit_activation: bfloat16 [2, 32, 3072], P('section', ('groups', 'expert', 'pair')), parts along dimension 1, may hold values from -6 to 6
- incoming_queue: bfloat16 [2, 32, 3072], P('section', ('groups', 'expert', 'pair')), parts along dimension 1, may hold values from -6 to 6
- expert_assignment: int32 [2, 3, 32, 1], P('section', None, ('groups', 'expert', 'pair')), parts along dimension 2, may hold values from 0 to 1; in each aligned block of 2 rows (0 to 1, 2 to 3, ..., all dimensions but the last counted through in order) at most 2 rows name the same one
- rescale_factor: float32 [2, 3072], P('section'), may hold values from 0.25 to 1.75
- routing_matrix: bfloat16 [2, 3072, 2], P('section'), may hold values from -0.109375 to 0.109375
- gating_matrix: bfloat16 [2, 2, 3072, 8192], P('section', 'pair', None, 'expert'), may hold values from -0.109375 to 0.109375
- expand_matrix: bfloat16 [2, 2, 3072, 8192], P('section', 'pair', None, 'expert'), may hold values from -0.109375 to 0.109375
- contract_matrix: bfloat16 [2, 2, 8192, 3072], P('section', 'pair', 'expert'), may hold values from -0.0625 to 0.0625
Outputs:
- inflight_out: bfloat16 [2, 32, 3072], P('section', ('groups', 'expert', 'pair')), parts along dimension 1
- finished: bfloat16 [2, 32, 3072], P('section', ('groups', 'expert', 'pair')), parts along dimension 1
The draws below stay inside these ranges and needn't reach their ends.
There are 2 independent parts, one for each index of `groups`. The reference program is written for one: setup_inputs(seed, part) draws one part's arguments, and reference() takes and returns one part's arrays. A program takes and returns all parts, laid end to end along the dimension named above; an argument that names none is the same for every part. Nothing has to cross between parts.
Inputs may be any that keep to these rules, and one draw needn't show every extreme that they name: `expert_assignment`: the expert chosen by each token of each layer and tick. In each aligned block of 2 rows, no expert is chosen by more than 2 rows.
All inputs are finite; a program needn't handle non-finite values.
Results may differ from the reference program's by a relative error of at most 0.023.
Values may be sent and summed in bfloat16 or wider, within the bound.
A program may use at most 64 MiB of HBM per device.

```python
import math
import jax
import jax.numpy as jnp
import numpy as np
from jax import lax

EMBED_DIMENSION = 3072
FF = 8192
EXPERTS = 2
TICKS = 3
TOK_DEV = 2
MICRO_COUNT = 16
CAP = 2
N_SECTION = 2
N_EXPERT = 4
N_PAIR = 2


def steps_of(own_key, dims, cuts, low, largest):
    def one(position, blocks):
        steps = jax.random.uniform(jax.random.fold_in(jax.random.fold_in(own_key, 6), position), (blocks,), jnp.float32, low / len(cuts), largest / len(cuts))
        return jnp.repeat(jnp.exp(steps), dims[position] // blocks).reshape((-1,) + (1,) * (len(dims) - position - 1))

    level = one(*cuts[0])
    for cut in cuts[1:]:
        level = level * one(*cut)
    return level


def assign_block(rng, own, number, rows, count, top, reach, lean):
    ranking = jax.random.permutation(rng, count)
    packed, common = shares(count, rows * top, reach, lean, True), shares(count, rows * top, reach, lean, False)
    places = jnp.arange(count)

    def named(sizes, rotation):
        used = int((sizes > 0).sum())
        fixed = max(1, used // 4)
        moved = fixed + (places - fixed + rotation * (used - fixed)) % max(1, count - fixed)
        return jnp.zeros((count,), jnp.int32).at[ranking[jnp.where(places < fixed, places, moved)]].set(jnp.asarray(sizes, jnp.int32))

    sizes = jnp.where(number % 4 == 0, named(packed, number // 4), named(common, number - number // 4 - 1))
    mixed = jax.random.permutation(jax.random.fold_in(own, 3), count)
    giver, sink = mixed[0:count // 2 * 2:2], mixed[1:count // 2 * 2:2]
    room = jnp.minimum(sizes[giver] - 1, reach - sizes[sink]) // 2
    room = jnp.where((giver == ranking[0]) | (sink == ranking[0]) | (sizes[sink] == 0), 0, jnp.maximum(room, 0))
    moved = jax.random.randint(jax.random.fold_in(own, 4), (count // 2,), 0, 1 << 20) % (room + 1)
    sizes = sizes.at[giver].add(-moved).at[sink].add(moved)
    members = jnp.searchsorted(jnp.cumsum(sizes), jnp.arange(rows * top), side="right").astype(jnp.int32)
    grid = members.reshape(top, rows).T
    grid = grid[jax.random.permutation(jax.random.fold_in(own, 1), rows)]
    rotation = jax.random.randint(jax.random.fold_in(own, 2), (rows, 1), 0, top)
    return jnp.take_along_axis(grid, (jnp.arange(top)[None, :] + rotation) % top, axis=1)


def shares(number_of, total, bound, skew, full):
    portions = [(1 << 20) // math.isqrt(grade ** skew) + 1 for grade in range(1, number_of + 1)]
    largest = bound if full else min(bound, max(-(-total // number_of), total * portions[0] // sum(portions)))
    least = 1 if total - largest >= number_of - 1 else 0
    counts, spare = [largest] + [least] * (number_of - 1), total - largest - least * (number_of - 1)
    while spare > 0:
        candidates = [i for i in range(1, number_of) if counts[i] < largest] or [i for i in range(1, number_of) if counts[i] < bound]
        pool, budget = sum([portions[i] for i in candidates]), spare
        for i in candidates:
            extra = min(bound - counts[i], max(1, budget * portions[i] // pool), spare)
            counts[i] = counts[i] + extra
            spare = spare - extra
    return np.array(counts)


def centred(rng, dims, scale, bound, cuts=(), kind=jnp.bfloat16):
    drawn = scale * jax.random.normal(rng, dims, jnp.float32)
    if cuts:
        drawn = drawn * steps_of(rng, dims, cuts, -0.22, 0.18)
    return jnp.clip(drawn, -bound, bound).astype(kind)


def setup_inputs(seed: int = 0, part: int = 0) -> dict:
    keys = jax.random.split(jax.random.key(seed), 9)
    part_keys = jax.random.split(jax.random.fold_in(keys[8], part), 9)
    transit_activation = centred(part_keys[0], (N_SECTION, MICRO_COUNT, EMBED_DIMENSION), 1.0, 6.0, ((0, 2), (1, 8)))
    incoming_queue = centred(part_keys[1], (N_SECTION, MICRO_COUNT, EMBED_DIMENSION), 1.0, 6.0, ((0, 2), (1, 8)))
    expert_assignment_keys = jax.random.split(jax.random.fold_in(part_keys[2], 1), N_SECTION * TICKS * MICRO_COUNT // TOK_DEV)
    expert_assignment_turns = jax.random.permutation(jax.random.fold_in(part_keys[2], 3), N_SECTION * TICKS * MICRO_COUNT // TOK_DEV)
    expert_assignment = jax.vmap(lambda own, number: assign_block(jax.random.fold_in(part_keys[2], 2), own, number, TOK_DEV, EXPERTS, 1, CAP, 2))(expert_assignment_keys, expert_assignment_turns).reshape((N_SECTION, TICKS, MICRO_COUNT, 1))
    rescale_factor = jnp.clip(1.0 + 0.15 * jax.random.normal(keys[3], (N_SECTION, EMBED_DIMENSION), jnp.float32), 0.25, 1.75)
    routing_matrix = centred(keys[4], (N_SECTION, EMBED_DIMENSION, EXPERTS), EMBED_DIMENSION ** -0.5, 0.109375, ((0, 2),))
    gating_matrix = centred(keys[5], (N_SECTION, EXPERTS, EMBED_DIMENSION, FF), EMBED_DIMENSION ** -0.5, 0.109375, ((0, 2), (1, 2), (3, 4)))
    expand_matrix = centred(keys[6], (N_SECTION, EXPERTS, EMBED_DIMENSION, FF), EMBED_DIMENSION ** -0.5, 0.109375, ((0, 2), (1, 2), (3, 4)))
    contract_matrix = centred(keys[7], (N_SECTION, EXPERTS, FF, EMBED_DIMENSION), FF ** -0.5, 0.0625, ((0, 2), (1, 2), (2, 4)))
    return dict(transit_activation=transit_activation, incoming_queue=incoming_queue, expert_assignment=expert_assignment, rescale_factor=rescale_factor, routing_matrix=routing_matrix, gating_matrix=gating_matrix, expand_matrix=expand_matrix, contract_matrix=contract_matrix)


def down_sum(hidden, down):
    part = FF // N_EXPERT

    def add(index, total):
        start = index.astype(jnp.int32) * part
        columns = lax.dynamic_slice_in_dim(hidden, start, part, 1)
        weights = lax.dynamic_slice_in_dim(down, start, part, 0)
        piece = jnp.dot(columns, weights, preferred_element_type=jnp.float32)
        return total + lax.optimization_barrier(piece.astype(jnp.bfloat16)).astype(jnp.float32)
    return lax.fori_loop(0, N_EXPERT, add, jnp.zeros((hidden.shape[0], EMBED_DIMENSION), jnp.float32))

def layer_apply(rows, picks, gain, table, gate_all, up_all, down_all):
    sources = N_EXPERT * N_PAIR
    wide = rows.astype(jnp.float32)
    square = lax.optimization_barrier(jnp.mean(wide * wide, axis=-1, keepdims=True))
    normed = (wide * lax.rsqrt(square + 1e-06) * gain).astype(jnp.bfloat16)
    logits = jnp.dot(normed, table, preferred_element_type=jnp.float32)
    chosen = jnp.take_along_axis(logits, picks, axis=1)[:, 0]
    other = jnp.take_along_axis(logits, (1 - picks).astype(jnp.int32), axis=1)[:, 0]
    weight = jax.nn.sigmoid(chosen - other)[:, None]
    pick = picks[:, 0].astype(jnp.int32)
    blocks = pick.reshape(sources, TOK_DEV)
    flags = (blocks[:, :, None] == jnp.arange(EXPERTS, dtype=jnp.int32)[None, None, :]).astype(jnp.int32)
    before = (jnp.cumsum(flags, axis=1) - flags).astype(jnp.int32)
    slot = lax.optimization_barrier(jnp.sum(before * flags, axis=-1)).reshape(-1).astype(jnp.int32)
    source = (jnp.arange(MICRO_COUNT, dtype=jnp.int32) // TOK_DEV).astype(jnp.int32)
    buffer = jnp.zeros((EXPERTS, sources, CAP, EMBED_DIMENSION), jnp.bfloat16).at[pick, source, slot].set(normed)
    answers = []
    for expert in range(EXPERTS):
        flat = buffer[expert].reshape(sources * CAP, EMBED_DIMENSION)
        gate = jnp.dot(flat, gate_all[expert], preferred_element_type=jnp.float32)
        upper = jnp.dot(flat, up_all[expert], preferred_element_type=jnp.float32)
        hidden = (jax.nn.silu(gate) * upper).astype(jnp.bfloat16)
        summed = down_sum(hidden, down_all[expert])
        answers.append(summed.astype(jnp.bfloat16).reshape(sources, CAP, EMBED_DIMENSION))
    answer = jnp.stack(answers)
    picked = answer[pick, source, slot].astype(jnp.float32)
    return (wide + weight * picked).astype(jnp.bfloat16)

def reference(transit_activation, incoming_queue, expert_assignment, rescale_factor, routing_matrix, gating_matrix, expand_matrix, contract_matrix):
    present_carry = [transit_activation[advance_level] for advance_level in range(N_SECTION)]
    side = [incoming_queue[advance_level] for advance_level in range(N_SECTION)]
    for tick in range(TICKS):
        for layer in range(N_SECTION):
            place = (layer - tick) % N_SECTION
            present_carry[place] = layer_apply(present_carry[place], expert_assignment[layer, tick], rescale_factor[layer], routing_matrix[layer], gating_matrix[layer], expand_matrix[layer], contract_matrix[layer])
        arriving = -(tick + 1) % N_SECTION
        present_carry[arriving], side[arriving] = (side[arriving], present_carry[arriving])
    held = [present_carry[(j - TICKS) % N_SECTION] for j in range(N_SECTION)]
    waiting = [side[(j - TICKS) % N_SECTION] for j in range(N_SECTION)]
    return (jnp.stack(held), jnp.stack(waiting))
```

```python
import functools

import jax
import jax.numpy as jnp
from jax import lax
from jax.experimental import pallas as pl
from jax.experimental.pallas import tpu as pltpu
from jax.sharding import PartitionSpec as P

EPSILON = 1e-06
F32 = jnp.float32
BF16 = jnp.bfloat16


def width_of(total, most):
    width = most
    while total % width:
        width -= 128
    return width


def window_kernel(
    sizes, act, queue, picks, gain, table, gate_hbm, up_hbm, down_hbm, inflight, finished, *scratch
):
    sections, experts_ax, pairs, ticks, tok, width, hidden_w, fw, dw, levels, pads = sizes
    n = experts_ax * pairs
    fc, dc = hidden_w // fw, width // dw
    it = iter(scratch)
    gate_w, up_w, down_w, w_sem = next(it), next(it), next(it), next(it)
    queue_in, q_send, q_recv = next(it), next(it), next(it)
    held, h_send, h_recv = next(it), next(it), next(it)
    end_now, end_side, end_send, end_recv = next(it), next(it), next(it), next(it)
    per_level = [tuple(next(it) for _ in range(11)) for _ in range(levels)]
    sec = lax.axis_index("section")
    my_e = lax.axis_index("expert")
    my_p = lax.axis_index("pair")
    me = my_e * pairs + my_p

    def fetch(kind, c):
        if kind == 0:
            src, dst = gate_hbm.at[0, 0, :, pl.ds(c * fw, fw)], gate_w.at[c]
        elif kind == 1:
            src, dst = up_hbm.at[0, 0, :, pl.ds(c * fw, fw)], up_w.at[c]
        else:
            src, dst = down_hbm.at[0, 0, :, pl.ds(c * dw, dw)], down_w.at[c]
        base = (0, fc, 2 * fc)[kind]
        return pltpu.make_async_copy(src, dst, w_sem.at[base + c])

    for c in range(fc):
        fetch(0, c).start()
        fetch(1, c).start()
    for c in range(dc):
        fetch(2, c).start()

    def peer_at(off):
        peer = lax.rem(me + off, n)
        return peer, {"expert": peer // pairs, "pair": lax.rem(peer, pairs)}

    barrier = pltpu.get_barrier_semaphore()

    def greet(off, carry):
        pl.semaphore_signal(barrier, inc=1, device_id=peer_at(off)[1])
        return carry

    lax.fori_loop(1, n, greet, 0)
    for off in range(1, sections):
        pl.semaphore_signal(barrier, inc=1, device_id={"section": lax.rem(sec + off, sections)})
    pl.semaphore_wait(barrier, n - 1 + sections - 1)

    for k in range(1, ticks):
        origin = sections - k
        if origin == 0:
            continue
        copy = pltpu.make_async_remote_copy(
            queue.at[0],
            queue_in.at[k - 1],
            q_send.at[k - 1],
            q_recv.at[k - 1],
            device_id={"section": 0},
        )

        @pl.when(sec == origin)
        def _():
            copy.start()

    def final_spot(k):
        place = ticks - 1 - k
        return (0, True) if place == sections else (place, False)

    movers = []
    if ticks <= sections:
        movers.append((sections - ticks, 0, True))
    for s in range(ticks, sections):
        movers.append((s - ticks, s, False))
    for origin, goal, now in movers:
        dst = end_now if now else end_side
        sem = 0 if now else 1
        if origin == goal:

            @pl.when(sec == origin)
            def _():
                dst[...] = queue[0]

        else:

            @pl.when(sec == origin)
            def _():
                pltpu.make_async_remote_copy(
                    queue.at[0],
                    dst,
                    end_send.at[2],
                    end_recv.at[sem],
                    device_id={"section": goal},
                ).start()

    rows_pick = lax.broadcasted_iota

    def level_work(level):
        count = ticks - level
        real = count * tok
        rows = pads[level]
        (x_send, xs_sem, xr_sem, x_all, lhs, h_all, p_send, ps_sem, pr_sem, p_all, res) = per_level[
            level
        ]
        if level == 0:
            blocks = [act[0].astype(F32)]
            for k in range(1, ticks):
                if sections - k == 0:
                    blocks.append(queue[0].astype(F32))
                else:

                    @pl.when(sec == 0)
                    def _():
                        pltpu.make_async_remote_copy(
                            queue.at[0],
                            queue_in.at[k - 1],
                            q_send.at[k - 1],
                            q_recv.at[k - 1],
                            device_id={"section": 1},
                        ).wait_recv()

                    @pl.when(sec != 0)
                    def _():
                        queue_in[k - 1] = jnp.zeros((tok, width), BF16)

                    blocks.append(queue_in[k - 1].astype(F32))
        else:
            for i in range(count):
                k = level + i

                def arrive():
                    pltpu.make_async_remote_copy(
                        res.at[i],
                        held.at[level - 1, i],
                        h_send.at[level - 1, i],
                        h_recv.at[level - 1, i],
                        device_id={"section": 0},
                    ).wait_recv()

                def blank():
                    held[level - 1, i] = jnp.zeros((tok, width), BF16)

                if i == 0:
                    arrive()
                else:
                    pl.when(sec == level)(arrive)
                    pl.when(sec != level)(blank)
            blocks = [held[level - 1, i].astype(F32) for i in range(count)]
        if rows > real:
            blocks.append(jnp.zeros((rows - real, width), F32))
        wide = jnp.concatenate(blocks, axis=0)
        square = jnp.mean(wide * wide, axis=-1, keepdims=True)
        normed = (wide * lax.rsqrt(square + EPSILON) * gain[...]).astype(BF16).astype(F32)
        tab = table[0].astype(F32)
        first = jnp.sum(normed * tab[0:1], axis=-1, keepdims=True)
        second = jnp.sum(normed * tab[1:2], axis=-1, keepdims=True)
        line = rows_pick(jnp.int32, (rows, 1), 0)
        pick = jnp.zeros((rows, 1), jnp.int32)
        for i in range(count):
            for t in range(tok):
                pick = jnp.where(line == i * tok + t, picks[0, level + i, t, 0], pick)
        delta = jnp.where(pick == 0, first - second, second - first)
        weight = 1.0 / (1.0 + jnp.exp(-delta))
        for p in range(pairs):
            x_send[p] = jnp.where(pick == p, normed, 0.0).astype(BF16)

        def x_copy(slot, peer, target):
            return pltpu.make_async_remote_copy(
                x_send.at[slot],
                x_all.at[me],
                xs_sem.at[peer],
                xr_sem.at[me],
                device_id=target,
            )

        def send_x(off, carry):
            peer, target = peer_at(off)
            x_copy(lax.rem(peer, pairs), peer, target).start()
            return carry

        lax.fori_loop(1, n, send_x, 0)
        x_all[me] = x_send[my_p]

        def take_x(off, carry):
            peer, target = peer_at(off)
            pltpu.make_async_remote_copy(
                x_send.at[0], x_all.at[peer], xs_sem.at[peer], xr_sem.at[peer], device_id=target
            ).wait_recv()
            return carry

        lax.fori_loop(1, n, take_x, 0)
        if rows % 8 == 0:
            lhs[...] = x_all[...].astype(F32).reshape(n * rows, width).astype(BF16)
        else:
            group = max(1, 16 // rows)
            for d in range(0, n, group):
                lhs[d * rows : (d + group) * rows] = jnp.concatenate(
                    [x_all[d + j].astype(F32) for j in range(group)], axis=0
                ).astype(BF16)

        def widen(c, carry):
            if level == 0:
                fetch(0, c).wait()
                fetch(1, c).wait()
            gate = jnp.dot(lhs[...], gate_w[c], preferred_element_type=F32)
            upper = jnp.dot(lhs[...], up_w[c], preferred_element_type=F32)
            h_all[c] = (gate / (1.0 + jnp.exp(-gate)) * upper).astype(BF16)
            return carry

        lax.fori_loop(0, fc, widen, 0)

        def p_copy(c, peer, target):
            return pltpu.make_async_remote_copy(
                p_send.at[c, peer],
                p_all.at[c, me],
                ps_sem.at[c, peer],
                pr_sem.at[c, me],
                device_id=target,
            )

        def narrow(c, carry):
            if level == 0:
                fetch(2, c).wait()
            part = jnp.zeros((n * rows, dw), F32)
            for i in range(fc):
                part = part + jnp.dot(
                    h_all[i], down_w[c, i * fw : (i + 1) * fw], preferred_element_type=F32
                )
            if rows % 8 == 0:
                p_send[c] = part.reshape(n, rows, dw).astype(BF16)
            else:
                for d in range(n):
                    p_send[c, d] = part[d * rows : (d + 1) * rows].astype(BF16)

            def send_p(off, inner):
                peer, target = peer_at(off)
                p_copy(c, peer, target).start()
                return inner

            lax.fori_loop(1, n, send_p, 0)
            p_all[c, me] = p_send[c, me]
            return carry

        lax.fori_loop(0, dc, narrow, 0)
        for c in range(dc):

            def take_p(off, carry):
                peer, target = peer_at(off)
                pltpu.make_async_remote_copy(
                    p_send.at[c, peer],
                    p_all.at[c, peer],
                    ps_sem.at[c, peer],
                    pr_sem.at[c, peer],
                    device_id=target,
                ).wait_recv()
                return carry

            lax.fori_loop(1, n, take_p, 0)
            total = jnp.sum(p_all[c].astype(F32), axis=0).astype(BF16).astype(F32)
            span = slice(c * dw, (c + 1) * dw)
            done = wide[:, span] + weight * total
            for i in range(count):
                res[i, :, span] = done[i * tok : (i + 1) * tok].astype(BF16)

        def goals(i):
            k = level + i
            place, now = final_spot(k)
            out = []
            if i == 0:
                middle = (sec >= level) & (sec < sections - 1)
            else:
                middle = (sec == level) & (sec < sections - 1)
            target = {"section": lax.rem(sec + 1, sections)}
            if k < ticks - 1:
                if level + 1 < levels:
                    out.append(
                        (
                            middle,
                            pltpu.make_async_remote_copy(
                                res.at[i],
                                held.at[level, i],
                                h_send.at[level, i],
                                h_recv.at[level, i],
                                device_id=target,
                            ),
                        )
                    )
            else:
                out.append(
                    (
                        middle,
                        pltpu.make_async_remote_copy(
                            res.at[i], end_now, h_send.at[level, i], end_recv.at[0], device_id=target
                        ),
                    )
                )
            if i == 0 or level == sections - 1:
                last = sec == sections - 1
                dst, sem = (end_now, 0) if now else (end_side, 1)
                if place == sections - 1 and not now:
                    out.append((last, None))
                else:
                    out.append(
                        (
                            last,
                            pltpu.make_async_remote_copy(
                                res.at[i],
                                dst,
                                h_send.at[level, i],
                                end_recv.at[sem],
                                device_id={"section": place},
                            ),
                        )
                    )
            return out

        for i in range(count):
            for condition, copy in goals(i):

                @pl.when(condition)
                def _():
                    if copy is None:
                        end_side[...] = res[i]
                    else:
                        copy.start()

        def settle(off, carry):
            peer, target = peer_at(off)
            x_copy(0, peer, target).wait_send()
            for c in range(dc):
                p_copy(c, peer, target).wait_send()
            return carry

        def finish():
            lax.fori_loop(1, n, settle, 0)
            for i in range(count):
                for condition, copy in goals(i):
                    if copy is not None:

                        @pl.when(condition)
                        def _():
                            copy.wait_send()

        return finish

    for level in range(levels):
        if level == 0:
            level_work(0)()
        else:

            @pl.when(sec >= level)
            def _():
                level_work(level)()

    for k in range(1, ticks):
        origin = sections - k
        if origin == 0:
            continue

        @pl.when(sec == origin)
        def _():
            pltpu.make_async_remote_copy(
                queue.at[0],
                queue_in.at[k - 1],
                q_send.at[k - 1],
                q_recv.at[k - 1],
                device_id={"section": 0},
            ).wait_send()

    for origin, goal, now in movers:
        if origin != goal:

            @pl.when(sec == origin)
            def _():
                pltpu.make_async_remote_copy(
                    queue.at[0],
                    end_now,
                    end_send.at[2],
                    end_recv.at[0],
                    device_id={"section": goal},
                ).wait_send()

    def land(dst, sem):
        pltpu.make_async_remote_copy(
            queue.at[0], dst, end_send.at[0], end_recv.at[sem], device_id={"section": 0}
        ).wait_recv()

    local_now = [goal for origin, goal, now in movers if now and origin == goal]
    if not local_now:
        land(end_now, 0)
    else:
        pl.when(sec != local_now[0])(lambda: land(end_now, 0))
    local_side = [goal for origin, goal, now in movers if not now and origin == goal]
    if ticks >= sections:
        local_side.append(sections - 1)
    remote = sec >= 0
    for goal in local_side:
        remote = remote & (sec != goal)
    pl.when(remote)(lambda: land(end_side, 1))
    inflight[0] = end_now[...]
    finished[0] = end_side[...]


def body(act, queue, picks, gain, table, gate_w, up_w, down_w):
    sections, experts_ax, pairs = (lax.axis_size(a) for a in ("section", "expert", "pair"))
    ticks, tok = picks.shape[1], picks.shape[2]
    width, hidden_w = gate_w.shape[2], gate_w.shape[3]
    n = experts_ax * pairs
    fw, dw = width_of(hidden_w, 512), width_of(width, 768)
    fc, dc = hidden_w // fw, width // dw
    levels = min(sections, ticks)
    assert ticks <= sections + 1
    pads = []
    for level in range(levels):
        real = (ticks - level) * tok
        pads.append(real if real in (1, 2, 4) else -(-real // 8) * 8)
    dma = pltpu.SemaphoreType.DMA
    vm = pltpu.VMEM
    scratch = [
        vm((fc, width, fw), BF16),
        vm((fc, width, fw), BF16),
        vm((dc, hidden_w, dw), BF16),
        dma((2 * fc + dc,)),
        vm((ticks, tok, width), BF16),
        dma((ticks,)),
        dma((ticks,)),
        vm((levels, ticks, tok, width), BF16),
        dma((levels, ticks)),
        dma((levels, ticks)),
        vm((tok, width), BF16),
        vm((tok, width), BF16),
        dma((3,)),
        dma((2,)),
    ]
    for level in range(levels):
        rows = pads[level]
        scratch += [
            vm((pairs, rows, width), BF16),
            dma((n,)),
            dma((n,)),
            vm((n, rows, width), BF16),
            vm((n * rows, width), BF16),
            vm((fc, n * rows, fw), BF16),
            vm((dc, n, rows, dw), BF16),
            dma((dc, n)),
            dma((dc, n)),
            vm((dc, n, rows, dw), BF16),
            vm((ticks - level, tok, width), BF16),
        ]
    sizes = (
        sections, experts_ax, pairs, ticks, tok, width, hidden_w, fw, dw, levels, tuple(pads)
    )
    in_vmem = pl.BlockSpec(memory_space=pltpu.VMEM)
    anywhere = pl.BlockSpec(memory_space=pl.ANY)
    return pl.pallas_call(
        functools.partial(window_kernel, sizes),
        out_shape=(
            jax.ShapeDtypeStruct(act.shape, BF16),
            jax.ShapeDtypeStruct(act.shape, BF16),
        ),
        in_specs=[
            in_vmem,
            in_vmem,
            pl.BlockSpec(memory_space=pltpu.SMEM),
            in_vmem,
            in_vmem,
            anywhere,
            anywhere,
            anywhere,
        ],
        out_specs=(in_vmem, in_vmem),
        scratch_shapes=scratch,
        compiler_params=pltpu.CompilerParams(
            collective_id=0, has_side_effects=True, vmem_limit_bytes=60 * 1024 * 1024
        ),
    )(act, queue, picks, gain, jnp.swapaxes(table, 1, 2), gate_w, up_w, down_w)


def solution(mesh):
    in_specs = (
        P("section", ("groups", "expert", "pair"), None),
        P("section", ("groups", "expert", "pair"), None),
        P("section", None, ("groups", "expert", "pair"), None),
        P("section", None),
        P("section", None, None),
        P("section", "pair", None, "expert"),
        P("section", "pair", None, "expert"),
        P("section", "pair", "expert", None),
    )
    out_specs = (
        P("section", ("groups", "expert", "pair"), None),
        P("section", ("groups", "expert", "pair"), None),
    )
    return jax.shard_map(body, mesh=mesh, in_specs=in_specs, out_specs=out_specs, check_vma=False)
```

```python
import functools

import jax
import jax.numpy as jnp
from jax import lax
from jax.experimental import pallas as pl
from jax.experimental.pallas import tpu as pltpu
from jax.sharding import PartitionSpec as P

EPSILON = 1e-06
F32 = jnp.float32
BF16 = jnp.bfloat16


def width_of(total, most):
    width = most
    while total % width:
        width -= 128
    return width


def window_kernel(
    sizes, act, queue, picks, gain, table, gate_hbm, up_hbm, down_hbm, inflight, finished, *scratch
):
    sections, chips, pairs, ticks, tok, width, hidden_w, fw, dw, levels = sizes
    fc, dc = hidden_w // fw, width // dw
    wide_row = width + 128
    it = iter(scratch)
    gate_w, up_w, down_w, w_sem = next(it), next(it), next(it), next(it)
    queue_in, q_send, q_recv = next(it), next(it), next(it)
    end_send, end_recv = next(it), next(it)
    last = tuple(next(it) for _ in range(6))
    per_level = [tuple(next(it) for _ in range(22)) for _ in range(levels)]
    sec = lax.axis_index("section")
    my_e = lax.axis_index("expert")
    my_p = lax.axis_index("pair")

    def fetch(kind, c):
        if kind == 0:
            src, dst = gate_hbm.at[0, 0, :, pl.ds(c * fw, fw)], gate_w.at[c]
        elif kind == 1:
            src, dst = up_hbm.at[0, 0, :, pl.ds(c * fw, fw)], up_w.at[c]
        else:
            src, dst = down_hbm.at[0, 0, :, pl.ds(c * dw, dw)], down_w.at[c]
        base = (0, fc, 2 * fc)[kind]
        return pltpu.make_async_copy(src, dst, w_sem.at[base + c])

    def next_section(off=1):
        return lax.rem(sec + off, sections)

    barrier = pltpu.get_barrier_semaphore()

    def greet(off, carry):
        pl.semaphore_signal(
            barrier,
            inc=1,
            device_id={
                "section": lax.rem(sec + off // chips, sections),
                "expert": lax.rem(my_e + lax.rem(off, chips), chips),
            },
        )
        return carry

    lax.fori_loop(1, sections * chips, greet, 0)
    for q in range(1, pairs):
        pl.semaphore_signal(barrier, inc=1, device_id={"pair": lax.rem(my_p + q, pairs)})
    for c in range(fc):
        fetch(0, c).start()
        fetch(1, c).start()
    for c in range(dc):
        fetch(2, c).start()
    pl.semaphore_wait(barrier, sections * chips - 1 + pairs - 1)

    def queue_copy(k):
        return pltpu.make_async_remote_copy(
            queue.at[0],
            queue_in.at[k - 1],
            q_send.at[k - 1],
            q_recv.at[k - 1],
            device_id={"section": 0},
        )

    for k in range(1, ticks):
        if sections - k > 0:
            pl.when(sec == sections - k)(queue_copy(k).start)

    movers = []
    if ticks <= sections:
        movers.append((sections - ticks, 0, True))
    for s in range(ticks, sections):
        movers.append((s - ticks, s, False))

    def mover_copy(goal, now):
        return pltpu.make_async_remote_copy(
            queue.at[0],
            end_recv_rows.at[0 if now else 1],
            end_send.at[0],
            end_recv.at[0 if now else 1],
            device_id={"section": goal},
        )

    end_recv_rows = next(it)
    for origin, goal, now in movers:
        if origin != goal:
            pl.when(sec == origin)(mover_copy(goal, now).start)

    def routes(level, i):
        k = level + i
        out = []
        if level <= sections - 2:
            fits = (sec >= level) if i == 0 else (sec == level)
            out.append((fits & (sec < sections - 1), False, next_section(), False))
        if i == 0 or level == sections - 1:
            place = ticks - 1 - k
            out.append(
                (sec == sections - 1, True, place % sections, place == sections - 1)
            )
        return out

    def slots(level, i, to_last):
        if to_last:
            return last, level + i
        return per_level[level][16:22], i

    def rest_copies(level, i, to_last, place, x_ref):
        w_out, r_send = per_level[level][12], per_level[level][13]
        (_, xs, ws, _, x_sem, weight_sem), at = slots(level, i, to_last)
        return (
            pltpu.make_async_remote_copy(
                x_ref, xs.at[at], r_send.at[i, 0], x_sem.at[at], device_id={"section": place}
            ),
            pltpu.make_async_remote_copy(
                w_out.at[i], ws.at[at], r_send.at[i, 1], weight_sem.at[at],
                device_id={"section": place},
            ),
        )

    def z_copy(level, i, c, j, to_last, place):
        z_send, z_sem = per_level[level][14], per_level[level][15]
        (parts, _, _, part_sem, _, _), at = slots(level, i, to_last)
        return pltpu.make_async_remote_copy(
            z_send.at[i, c, j],
            parts.at[at, c, my_e],
            z_sem.at[i, c, j],
            part_sem.at[at, c, my_e],
            device_id={"section": place, "expert": j},
        )

    def combine(bufs, at, own, store):
        parts, xs, ws, part_sem, x_sem, weight_sem = bufs
        aside = {"section": next_section()}
        if not own:
            pltpu.make_async_remote_copy(
                xs.at[at], xs.at[at], end_send.at[1], x_sem.at[at], device_id=aside
            ).wait_recv()
            pltpu.make_async_remote_copy(
                ws.at[at], ws.at[at], end_send.at[1], weight_sem.at[at], device_id=aside
            ).wait_recv()
        for c in range(dc):

            def take(off, carry):
                j = lax.rem(my_e + off, chips)
                pltpu.make_async_remote_copy(
                    parts.at[at, c, j],
                    parts.at[at, c, j],
                    end_send.at[1],
                    part_sem.at[at, c, j],
                    device_id=aside,
                ).wait_recv()
                return carry

            lax.fori_loop(1 if own else 0, chips, take, 0)
            total = jnp.sum(parts[at, c].astype(F32), axis=0).astype(BF16).astype(F32)
            span = slice(c * dw, (c + 1) * dw)
            done = xs[at, :, span].astype(F32) + ws[at][:, 0:1] * total
            store(span, done.astype(BF16))

    def level_work(level):
        count = ticks - level
        real = count * tok
        pad = -(-real // 8) * 8
        half = count * chips * tok
        (
            x_in, x_send, x_all, xs_sem, xf_sem, xr_sem, lhs, h_all, s_buf, d_buf, ds_sem, dr_sem,
            w_out, r_send, z_send, z_sem,
        ) = per_level[level][:16]
        if level == 0:
            x_in[0] = act[0]
            for k in range(1, ticks):
                if sections - k == 0:
                    x_in[k] = queue[0]
                else:

                    @pl.when(sec == 0)
                    def _():
                        queue_copy(k).wait_recv()
                        x_in[k] = queue_in[k - 1]

                    @pl.when(sec != 0)
                    def _():
                        x_in[k] = jnp.zeros((tok, width), BF16)

        else:
            for i in range(count):

                def arrive():
                    def store(span, rows):
                        x_in[i, :, span] = rows

                    combine(per_level[level - 1][16:22], i, False, store)

                if i == 0:
                    arrive()
                else:
                    pl.when(sec == level)(arrive)

                    @pl.when(sec != level)
                    def _():
                        x_in[i] = jnp.zeros((tok, width), BF16)

        blocks = [x_in[i].astype(F32) for i in range(count)]
        if pad > real:
            blocks.append(jnp.zeros((pad - real, width), F32))
        wide = jnp.concatenate(blocks, axis=0)
        square = jnp.mean(wide * wide, axis=-1, keepdims=True)
        normed = (wide * lax.rsqrt(square + EPSILON) * gain[...]).astype(BF16).astype(F32)
        line = lax.broadcasted_iota(jnp.int32, (pad, 1), 0)
        pick = jnp.zeros((pad, 1), jnp.int32)
        for i in range(count):
            for t in range(tok):
                pick = jnp.where(line == i * tok + t, picks[0, t, 0, level + i], pick)
        flag = jnp.broadcast_to(pick.astype(F32), (pad, 128))
        for i in range(count):
            x_send[i, :, 0:width] = normed[i * tok : (i + 1) * tok].astype(BF16)
            x_send[i, :, width:wide_row] = flag[i * tok : (i + 1) * tok].astype(BF16)

        def across(off):
            j = lax.rem(my_e + off, chips)
            return pltpu.make_async_remote_copy(
                x_send,
                x_all.at[my_e, my_p],
                xs_sem.at[j],
                xr_sem.at[my_e, my_p],
                device_id={"expert": j},
            )

        def beside(off, q):
            j = lax.rem(my_e + off, chips)
            return pltpu.make_async_remote_copy(
                x_send if isinstance(off, int) else x_all.at[j, my_p],
                x_all.at[j, my_p],
                xf_sem.at[j, q - 1],
                xr_sem.at[j, my_p],
                device_id={"pair": lax.rem(my_p + q, pairs)},
            )

        def arrived(j, p):
            pltpu.make_async_remote_copy(
                x_send, x_all.at[j, p], xs_sem.at[0], xr_sem.at[j, p],
                device_id={"section": next_section()},
            ).wait_recv()

        def go(off, carry):
            across(off).start()
            return carry

        lax.fori_loop(1, chips, go, 0)
        for q in range(1, pairs):
            beside(0, q).start()
        x_all[my_e, my_p] = x_send[...]
        tab = table[0].astype(F32)
        first = jnp.sum(normed * tab[0:1], axis=-1, keepdims=True)
        second = jnp.sum(normed * tab[1:2], axis=-1, keepdims=True)
        delta = jnp.where(pick == 0, first - second, second - first)
        weight = jnp.broadcast_to(1.0 / (1.0 + jnp.exp(-delta)), (pad, 128))
        for i in range(count):
            w_out[i] = weight[i * tok : (i + 1) * tok]

        def relay(off, carry):
            j = lax.rem(my_e + off, chips)
            arrived(j, my_p)
            for q in range(1, pairs):
                beside(off, q).start()
            return carry

        lax.fori_loop(1, chips, relay, 0)
        for i in range(count):
            for condition, to_last, place, own in routes(level, i):

                @pl.when(condition)
                def _():
                    if own:
                        bufs, at = slots(level, i, to_last)
                        bufs[1][at] = x_in[i]
                        bufs[2][at] = w_out[i]
                    else:
                        for copy in rest_copies(level, i, to_last, place, x_in.at[i]):
                            copy.start()

        def gather(off, carry):
            j = lax.rem(my_e + off, chips)
            for q in range(1, pairs):
                arrived(j, lax.rem(my_p + q, pairs))
            return carry

        lax.fori_loop(0, chips, gather, 0)
        order = [(p, i, e) for p in range(pairs) for i in range(count) for e in range(chips)]
        group = max(1, 16 // tok)
        for start in range(0, len(order), group):
            rows = jnp.concatenate(
                [x_all[e, p, i].astype(F32) for p, i, e in order[start : start + group]], axis=0
            )
            mine = rows[:, width : width + 1] == my_p.astype(F32)
            lhs[start * tok : (start + group) * tok] = jnp.where(
                mine, rows[:, 0:width], 0.0
            ).astype(BF16)

        def widen(c, carry):
            if level == 0:
                fetch(0, c).wait()
                fetch(1, c).wait()
            gate = jnp.dot(lhs[...], gate_w[c], preferred_element_type=F32)
            upper = jnp.dot(lhs[...], up_w[c], preferred_element_type=F32)
            h_all[c] = (gate / (1.0 + jnp.exp(-gate)) * upper).astype(BF16)
            return carry

        lax.fori_loop(0, fc, widen, 0)

        def trade(c, q):
            other = lax.rem(my_p + q, pairs)
            return pltpu.make_async_remote_copy(
                s_buf.at[c, other],
                d_buf.at[c, pairs - 1 - q],
                ds_sem.at[c, q - 1],
                dr_sem.at[c, pairs - 1 - q],
                device_id={"pair": other},
            )

        def send_parts(i, c):
            for condition, to_last, place, own in routes(level, i):

                def send(off, carry):
                    z_copy(level, i, c, lax.rem(my_e + off, chips), to_last, place).start()
                    return carry

                @pl.when(condition)
                def _():
                    if own:
                        bufs, at = slots(level, i, to_last)
                        bufs[0][at, c, my_e] = z_send[i, c, my_e]
                    lax.fori_loop(1 if own else 0, chips, send, 0)

        early = count if level == levels - 1 else count - 1

        def ship(c):
            total = s_buf[c, my_p].astype(F32)
            for q in range(1, pairs):
                trade(c, q).wait_recv()
            for q in range(1, pairs):
                total = total + d_buf[c, q - 1].astype(F32)
            for i in range(count):
                for e in range(chips):
                    at = (i * chips + e) * tok
                    z_send[i, c, e] = total[at : at + tok].astype(BF16)
            for i in range(early):
                send_parts(i, c)

        for c in range(dc):
            if level == 0:
                fetch(2, c).wait()
            part = jnp.dot(h_all[0], down_w[c, 0:fw], preferred_element_type=F32)
            for i in range(1, fc):
                part = part + jnp.dot(
                    h_all[i], down_w[c, i * fw : (i + 1) * fw], preferred_element_type=F32
                )
            for p in range(pairs):
                s_buf[c, p] = part[p * half : (p + 1) * half].astype(BF16)
            for q in range(1, pairs):
                trade(c, q).start()
            if c > 0:
                ship(c - 1)
        ship(dc - 1)
        for i in range(early, count):
            for c in range(dc):
                send_parts(i, c)

        def settle():
            def out(off, carry):
                across(off).wait_send()
                return carry

            lax.fori_loop(1, chips, out, 0)
            for q in range(1, pairs):

                def forwarded(off, carry):
                    beside(off, q).wait_send()
                    return carry

                beside(0, q).wait_send()
                lax.fori_loop(1, chips, forwarded, 0)
                for c in range(dc):
                    trade(c, q).wait_send()
            for i in range(count):
                for condition, to_last, place, own in routes(level, i):

                    @pl.when(condition)
                    def _():
                        if not own:
                            for copy in rest_copies(level, i, to_last, place, x_in.at[i]):
                                copy.wait_send()
                        for c in range(dc):

                            def sent(off, carry):
                                j = lax.rem(my_e + off, chips)
                                z_copy(level, i, c, j, to_last, place).wait_send()
                                return carry

                            lax.fori_loop(1 if own else 0, chips, sent, 0)

        return settle

    settles = []
    for level in range(levels):
        if level == 0:
            settles.append(level_work(0))
        else:

            @pl.when(sec >= level)
            def _():
                settles.append(level_work(level))

    def to_inflight(span, rows):
        inflight[0, :, span] = rows

    def to_finished(span, rows):
        finished[0, :, span] = rows

    for level in range(levels):
        if level > sections - 2:
            continue
        source = sec - 1
        fits = (source >= level) if level == ticks - 1 else (source == level)

        @pl.when(fits)
        def _():
            combine(per_level[level][16:22], ticks - 1 - level, False, to_inflight)

    for k in range(ticks):
        place = ticks - 1 - k

        @pl.when(sec == place % sections)
        def _():
            combine(last, k, place == sections - 1, to_inflight if place == sections else to_finished)

    for origin, goal, now in movers:
        target = inflight if now else finished
        if origin == goal:

            @pl.when(sec == origin)
            def _():
                target[0] = queue[0]

        else:

            @pl.when(sec == goal)
            def _():
                mover_copy(goal, now).wait_recv()
                target[0] = end_recv_rows[0 if now else 1]

            pl.when(sec == origin)(mover_copy(goal, now).wait_send)

    for k in range(1, ticks):
        if sections - k > 0:
            pl.when(sec == sections - k)(queue_copy(k).wait_send)
    for level in range(levels):
        if level == 0:
            settles[0]()
        else:
            pl.when(sec >= level)(settles[level])


def body(act, queue, picks, gain, table, gate_w, up_w, down_w):
    sections, experts_ax, pairs = (lax.axis_size(a) for a in ("section", "expert", "pair"))
    ticks, tok = picks.shape[1], picks.shape[2]
    width, hidden_w = gate_w.shape[2], gate_w.shape[3]
    fw, dw = width_of(hidden_w, 512), width_of(width, 768)
    fc, dc = hidden_w // fw, width // dw
    levels = min(sections, ticks)
    assert ticks <= sections + 1
    chips = experts_ax
    dma = pltpu.SemaphoreType.DMA
    vm = pltpu.VMEM

    def landing(count):
        return [
            vm((count, dc, chips, tok, dw), BF16),
            vm((count, tok, width), BF16),
            vm((count, tok, 128), F32),
            dma((count, dc, chips)),
            dma((count,)),
            dma((count,)),
        ]

    scratch = [
        vm((fc, width, fw), BF16),
        vm((fc, width, fw), BF16),
        vm((dc, hidden_w, dw), BF16),
        dma((2 * fc + dc,)),
        vm((ticks, tok, width), BF16),
        dma((ticks,)),
        dma((ticks,)),
        dma((2,)),
        dma((2,)),
    ] + landing(ticks)
    others = max(1, pairs - 1)
    for level in range(levels):
        count = ticks - level
        half = count * chips * tok
        scratch += [
            vm((count, tok, width), BF16),
            vm((count, tok, width + 128), BF16),
            vm((chips, pairs, count, tok, width + 128), BF16),
            dma((chips,)),
            dma((chips, others)),
            dma((chips, pairs)),
            vm((pairs * half, width), BF16),
            vm((fc, pairs * half, fw), BF16),
            vm((dc, pairs, half, dw), BF16),
            vm((dc, others, half, dw), BF16),
            dma((dc, others)),
            dma((dc, others)),
            vm((count, tok, 128), F32),
            dma((count, 2)),
            vm((count, dc, chips, tok, dw), BF16),
            dma((count, dc, chips)),
        ] + landing(count)
    scratch.append(vm((2, tok, width), BF16))
    sizes = (sections, chips, pairs, ticks, tok, width, hidden_w, fw, dw, levels)
    in_vmem = pl.BlockSpec(memory_space=pltpu.VMEM)
    anywhere = pl.BlockSpec(memory_space=pl.ANY)
    return pl.pallas_call(
        functools.partial(window_kernel, sizes),
        out_shape=(
            jax.ShapeDtypeStruct(act.shape, BF16),
            jax.ShapeDtypeStruct(act.shape, BF16),
        ),
        in_specs=[
            in_vmem,
            in_vmem,
            pl.BlockSpec(memory_space=pltpu.SMEM),
            in_vmem,
            in_vmem,
            anywhere,
            anywhere,
            anywhere,
        ],
        out_specs=(in_vmem, in_vmem),
        scratch_shapes=scratch,
        compiler_params=pltpu.CompilerParams(
            collective_id=0, has_side_effects=True, vmem_limit_bytes=60 * 1024 * 1024
        ),
    )(act, queue, jnp.transpose(picks, (0, 2, 3, 1)), gain, jnp.swapaxes(table, 1, 2), gate_w, up_w, down_w)


def solution(mesh):
    in_specs = (
        P("section", ("groups", "expert", "pair"), None),
        P("section", ("groups", "expert", "pair"), None),
        P("section", None, ("groups", "expert", "pair"), None),
        P("section", None),
        P("section", None, None),
        P("section", "pair", None, "expert"),
        P("section", "pair", None, "expert"),
        P("section", "pair", "expert", None),
    )
    out_specs = (
        P("section", ("groups", "expert", "pair"), None),
        P("section", ("groups", "expert", "pair"), None),
    )
    return jax.shard_map(body, mesh=mesh, in_specs=in_specs, out_specs=out_specs, check_vma=False)
```

```python
import functools

import jax
import jax.numpy as jnp
from jax import lax
from jax.experimental import pallas as pl
from jax.experimental.pallas import tpu as pltpu
from jax.sharding import PartitionSpec as P

EPSILON = 1e-06
F32 = jnp.float32
BF16 = jnp.bfloat16


def width_of(total, most):
    width = most
    while total % width:
        width -= 128
    return width


def window_kernel(
    sizes, act, queue, picks, gain, table, gate_hbm, up_hbm, down_hbm, out, *scratch
):
    inflight, finished = out.at[0:1], out.at[1:2]
    sections, chips, pairs, ticks, tok, width, hidden_w, fw, dw, levels = sizes
    fc, dc = hidden_w // fw, width // dw
    wide_row = width + 128
    it = iter(scratch)
    gate_w, up_w, down_w, w_sem = next(it), next(it), next(it), next(it)
    queue_in, q_send, q_recv = next(it), next(it), next(it)
    end_send, end_recv = next(it), next(it)
    last = tuple(next(it) for _ in range(6))
    per_level = [tuple(next(it) for _ in range(22)) for _ in range(levels)]
    sec = lax.axis_index("section")
    my_e = lax.axis_index("expert")
    my_p = lax.axis_index("pair")

    def fetch(kind, c):
        if kind == 0:
            src, dst = gate_hbm.at[0, 0, :, pl.ds(c * fw, fw)], gate_w.at[c]
        elif kind == 1:
            src, dst = up_hbm.at[0, 0, :, pl.ds(c * fw, fw)], up_w.at[c]
        else:
            src, dst = down_hbm.at[0, 0, :, pl.ds(c * dw, dw)], down_w.at[c]
        base = (0, fc, 2 * fc)[kind]
        return pltpu.make_async_copy(src, dst, w_sem.at[base + c])

    def next_section(off=1):
        return lax.rem(sec + off, sections)

    barrier = pltpu.get_barrier_semaphore()

    def greet(off, carry):
        pl.semaphore_signal(
            barrier,
            inc=1,
            device_id={
                "section": lax.rem(sec + off // chips, sections),
                "expert": lax.rem(my_e + lax.rem(off, chips), chips),
            },
        )
        return carry

    lax.fori_loop(1, sections * chips, greet, 0)
    for q in range(1, pairs):
        pl.semaphore_signal(barrier, inc=1, device_id={"pair": lax.rem(my_p + q, pairs)})
    for c in range(fc):
        fetch(0, c).start()
        fetch(1, c).start()
    for c in range(dc):
        fetch(2, c).start()
    pl.semaphore_wait(barrier, sections * chips - 1 + pairs - 1)

    def queue_copy(k):
        return pltpu.make_async_remote_copy(
            queue.at[0],
            queue_in.at[k - 1],
            q_send.at[k - 1],
            q_recv.at[k - 1],
            device_id={"section": 0},
        )

    for k in range(1, ticks):
        if sections - k > 0:
            pl.when(sec == sections - k)(queue_copy(k).start)

    movers = []
    if ticks <= sections:
        movers.append((sections - ticks, 0, True))
    for s in range(ticks, sections):
        movers.append((s - ticks, s, False))

    def mover_copy(goal, now):
        return pltpu.make_async_remote_copy(
            queue.at[0],
            end_recv_rows.at[0 if now else 1],
            end_send.at[0],
            end_recv.at[0 if now else 1],
            device_id={"section": goal},
        )

    end_recv_rows = next(it)
    for origin, goal, now in movers:
        if origin != goal:
            pl.when(sec == origin)(mover_copy(goal, now).start)

    def routes(level, i):
        k = level + i
        out = []
        if level <= sections - 2:
            fits = (sec >= level) if i == 0 else (sec == level)
            out.append((fits & (sec < sections - 1), False, next_section(), False))
        if i == 0 or level == sections - 1:
            place = ticks - 1 - k
            out.append(
                (sec == sections - 1, True, place % sections, place == sections - 1)
            )
        return out

    def slots(level, i, to_last):
        if to_last:
            return last, level + i
        return per_level[level][16:22], i

    def rest_copies(level, i, to_last, place, x_ref):
        w_out, r_send = per_level[level][12], per_level[level][13]
        (_, xs, ws, _, x_sem, weight_sem), at = slots(level, i, to_last)
        return (
            pltpu.make_async_remote_copy(
                x_ref, xs.at[at], r_send.at[i, 0], x_sem.at[at], device_id={"section": place}
            ),
            pltpu.make_async_remote_copy(
                w_out.at[i], ws.at[at], r_send.at[i, 1], weight_sem.at[at],
                device_id={"section": place},
            ),
        )

    def z_copy(level, i, c, j, to_last, place):
        z_send, z_sem = per_level[level][14], per_level[level][15]
        (parts, _, _, part_sem, _, _), at = slots(level, i, to_last)
        return pltpu.make_async_remote_copy(
            z_send.at[i, c, j],
            parts.at[at, c, my_e],
            z_sem.at[i, c, j],
            part_sem.at[at, c, my_e],
            device_id={"section": place, "expert": j},
        )

    def combine(bufs, at, own, store):
        parts, xs, ws, part_sem, x_sem, weight_sem = bufs
        aside = {"section": next_section()}
        if not own:
            pltpu.make_async_remote_copy(
                xs.at[at], xs.at[at], end_send.at[1], x_sem.at[at], device_id=aside
            ).wait_recv()
            pltpu.make_async_remote_copy(
                ws.at[at], ws.at[at], end_send.at[1], weight_sem.at[at], device_id=aside
            ).wait_recv()
        for c in range(dc):

            def take(off, carry):
                j = lax.rem(my_e + off, chips)
                pltpu.make_async_remote_copy(
                    parts.at[at, c, j],
                    parts.at[at, c, j],
                    end_send.at[1],
                    part_sem.at[at, c, j],
                    device_id=aside,
                ).wait_recv()
                return carry

            lax.fori_loop(1 if own else 0, chips, take, 0)
            total = jnp.sum(parts[at, c].astype(F32), axis=0).astype(BF16).astype(F32)
            span = slice(c * dw, (c + 1) * dw)
            done = xs[at, :, span].astype(F32) + ws[at][:, 0:1] * total
            store(span, done.astype(BF16))

    def level_work(level):
        count = ticks - level
        real = count * tok
        pad = -(-real // 8) * 8
        half = count * chips * tok
        (
            x_in, x_send, x_all, xs_sem, xf_sem, xr_sem, lhs, h_all, s_buf, d_buf, ds_sem, dr_sem,
            w_out, r_send, z_send, z_sem,
        ) = per_level[level][:16]
        if level == 0:
            x_in[0] = act[0]
            for k in range(1, ticks):
                if sections - k == 0:
                    x_in[k] = queue[0]
                else:

                    @pl.when(sec == 0)
                    def _():
                        queue_copy(k).wait_recv()
                        x_in[k] = queue_in[k - 1]

                    @pl.when(sec != 0)
                    def _():
                        x_in[k] = jnp.zeros((tok, width), BF16)

        else:
            for i in range(count):

                def arrive():
                    def store(span, rows):
                        x_in[i, :, span] = rows

                    combine(per_level[level - 1][16:22], i, False, store)

                if i == 0:
                    arrive()
                else:
                    pl.when(sec == level)(arrive)

                    @pl.when(sec != level)
                    def _():
                        x_in[i] = jnp.zeros((tok, width), BF16)

        blocks = [x_in[i].astype(F32) for i in range(count)]
        if pad > real:
            blocks.append(jnp.zeros((pad - real, width), F32))
        wide = jnp.concatenate(blocks, axis=0)
        square = jnp.mean(wide * wide, axis=-1, keepdims=True)
        normed = (wide * lax.rsqrt(square + EPSILON) * gain[...]).astype(BF16).astype(F32)
        line = lax.broadcasted_iota(jnp.int32, (pad, 1), 0)
        pick = jnp.zeros((pad, 1), jnp.int32)
        for i in range(count):
            for t in range(tok):
                pick = jnp.where(line == i * tok + t, picks[0, t, 0, level + i], pick)
        flag = jnp.broadcast_to(pick.astype(F32), (pad, 128))
        for i in range(count):
            x_send[i, :, 0:width] = normed[i * tok : (i + 1) * tok].astype(BF16)
            x_send[i, :, width:wide_row] = flag[i * tok : (i + 1) * tok].astype(BF16)

        def across(off):
            j = lax.rem(my_e + off, chips)
            return pltpu.make_async_remote_copy(
                x_send,
                x_all.at[my_e, my_p],
                xs_sem.at[j],
                xr_sem.at[my_e, my_p],
                device_id={"expert": j},
            )

        def beside(off, q):
            j = lax.rem(my_e + off, chips)
            return pltpu.make_async_remote_copy(
                x_send if isinstance(off, int) else x_all.at[j, my_p],
                x_all.at[j, my_p],
                xf_sem.at[j, q - 1],
                xr_sem.at[j, my_p],
                device_id={"pair": lax.rem(my_p + q, pairs)},
            )

        def arrived(j, p):
            pltpu.make_async_remote_copy(
                x_send, x_all.at[j, p], xs_sem.at[0], xr_sem.at[j, p],
                device_id={"section": next_section()},
            ).wait_recv()

        def go(off, carry):
            across(off).start()
            return carry

        lax.fori_loop(1, chips, go, 0)
        for q in range(1, pairs):
            beside(0, q).start()
        x_all[my_e, my_p] = x_send[...]
        tab = table[0].astype(F32)
        first = jnp.sum(normed * tab[0:1], axis=-1, keepdims=True)
        second = jnp.sum(normed * tab[1:2], axis=-1, keepdims=True)
        delta = jnp.where(pick == 0, first - second, second - first)
        weight = jnp.broadcast_to(1.0 / (1.0 + jnp.exp(-delta)), (pad, 128))
        for i in range(count):
            w_out[i] = weight[i * tok : (i + 1) * tok]

        def relay(off, carry):
            j = lax.rem(my_e + off, chips)
            arrived(j, my_p)
            for q in range(1, pairs):
                beside(off, q).start()
            return carry

        lax.fori_loop(1, chips, relay, 0)
        for i in range(count):
            for condition, to_last, place, own in routes(level, i):

                @pl.when(condition)
                def _():
                    if own:
                        bufs, at = slots(level, i, to_last)
                        bufs[1][at] = x_in[i]
                        bufs[2][at] = w_out[i]
                    else:
                        for copy in rest_copies(level, i, to_last, place, x_in.at[i]):
                            copy.start()

        def gather(off, carry):
            j = lax.rem(my_e + off, chips)
            for q in range(1, pairs):
                arrived(j, lax.rem(my_p + q, pairs))
            return carry

        lax.fori_loop(0, chips, gather, 0)
        order = [(p, i, e) for p in range(pairs) for i in range(count) for e in range(chips)]
        group = max(1, 16 // tok)
        for start in range(0, len(order), group):
            rows = jnp.concatenate(
                [x_all[e, p, i].astype(F32) for p, i, e in order[start : start + group]], axis=0
            )
            mine = rows[:, width : width + 1] == my_p.astype(F32)
            lhs[start * tok : (start + group) * tok] = jnp.where(
                mine, rows[:, 0:width], 0.0
            ).astype(BF16)

        def widen(c, carry):
            if level == 0:
                fetch(0, c).wait()
                fetch(1, c).wait()
            gate = jnp.dot(lhs[...], gate_w[c], preferred_element_type=F32)
            upper = jnp.dot(lhs[...], up_w[c], preferred_element_type=F32)
            h_all[c] = (gate / (1.0 + jnp.exp(-gate)) * upper).astype(BF16)
            return carry

        lax.fori_loop(0, fc, widen, 0)

        def trade(c, q):
            other = lax.rem(my_p + q, pairs)
            return pltpu.make_async_remote_copy(
                s_buf.at[c, other],
                d_buf.at[c, pairs - 1 - q],
                ds_sem.at[c, q - 1],
                dr_sem.at[c, pairs - 1 - q],
                device_id={"pair": other},
            )

        def send_parts(i, c):
            for condition, to_last, place, own in routes(level, i):

                def send(off, carry):
                    z_copy(level, i, c, lax.rem(my_e + off, chips), to_last, place).start()
                    return carry

                @pl.when(condition)
                def _():
                    if own:
                        bufs, at = slots(level, i, to_last)
                        bufs[0][at, c, my_e] = z_send[i, c, my_e]
                    lax.fori_loop(1 if own else 0, chips, send, 0)

        early = count if level == levels - 1 else count - 1

        def ship(c):
            total = s_buf[c, my_p].astype(F32)
            for q in range(1, pairs):
                trade(c, q).wait_recv()
            for q in range(1, pairs):
                total = total + d_buf[c, q - 1].astype(F32)
            for i in range(count):
                for e in range(chips):
                    at = (i * chips + e) * tok
                    z_send[i, c, e] = total[at : at + tok].astype(BF16)
            for i in range(early):
                send_parts(i, c)

        for c in range(dc):
            if level == 0:
                fetch(2, c).wait()
            part = jnp.dot(h_all[0], down_w[c, 0:fw], preferred_element_type=F32)
            for i in range(1, fc):
                part = part + jnp.dot(
                    h_all[i], down_w[c, i * fw : (i + 1) * fw], preferred_element_type=F32
                )
            for p in range(pairs):
                s_buf[c, p] = part[p * half : (p + 1) * half].astype(BF16)
            for q in range(1, pairs):
                trade(c, q).start()
            if c > 0:
                ship(c - 1)
        ship(dc - 1)
        for i in range(early, count):
            for c in range(dc):
                send_parts(i, c)

        def settle():
            def out(off, carry):
                across(off).wait_send()
                return carry

            lax.fori_loop(1, chips, out, 0)
            for q in range(1, pairs):

                def forwarded(off, carry):
                    beside(off, q).wait_send()
                    return carry

                beside(0, q).wait_send()
                lax.fori_loop(1, chips, forwarded, 0)
                for c in range(dc):
                    trade(c, q).wait_send()
            for i in range(count):
                for condition, to_last, place, own in routes(level, i):

                    @pl.when(condition)
                    def _():
                        if not own:
                            for copy in rest_copies(level, i, to_last, place, x_in.at[i]):
                                copy.wait_send()
                        for c in range(dc):

                            def sent(off, carry):
                                j = lax.rem(my_e + off, chips)
                                z_copy(level, i, c, j, to_last, place).wait_send()
                                return carry

                            lax.fori_loop(1 if own else 0, chips, sent, 0)

        return settle

    settles = []
    for level in range(levels):
        if level == 0:
            settles.append(level_work(0))
        else:

            @pl.when(sec >= level)
            def _():
                settles.append(level_work(level))

    def to_inflight(span, rows):
        inflight[0, :, span] = rows

    def to_finished(span, rows):
        finished[0, :, span] = rows

    for level in range(levels):
        if level > sections - 2:
            continue
        source = sec - 1
        fits = (source >= level) if level == ticks - 1 else (source == level)

        @pl.when(fits)
        def _():
            combine(per_level[level][16:22], ticks - 1 - level, False, to_inflight)

    for k in range(ticks):
        place = ticks - 1 - k

        @pl.when(sec == place % sections)
        def _():
            combine(last, k, place == sections - 1, to_inflight if place == sections else to_finished)

    for origin, goal, now in movers:
        target = inflight if now else finished
        if origin == goal:

            @pl.when(sec == origin)
            def _():
                target[0] = queue[0]

        else:

            @pl.when(sec == goal)
            def _():
                mover_copy(goal, now).wait_recv()
                target[0] = end_recv_rows[0 if now else 1]

            pl.when(sec == origin)(mover_copy(goal, now).wait_send)

    for k in range(1, ticks):
        if sections - k > 0:
            pl.when(sec == sections - k)(queue_copy(k).wait_send)
    for level in range(levels):
        if level == 0:
            settles[0]()
        else:
            pl.when(sec >= level)(settles[level])


def body(act, queue, picks, gain, table, gate_w, up_w, down_w):
    sections, experts_ax, pairs = (lax.axis_size(a) for a in ("section", "expert", "pair"))
    ticks, tok = picks.shape[1], picks.shape[2]
    width, hidden_w = gate_w.shape[2], gate_w.shape[3]
    fw, dw = width_of(hidden_w, 512), width_of(width, 768)
    fc, dc = hidden_w // fw, width // dw
    levels = min(sections, ticks)
    assert ticks <= sections + 1
    chips = experts_ax
    dma = pltpu.SemaphoreType.DMA
    vm = pltpu.VMEM

    def landing(count):
        return [
            vm((count, dc, chips, tok, dw), BF16),
            vm((count, tok, width), BF16),
            vm((count, tok, 128), F32),
            dma((count, dc, chips)),
            dma((count,)),
            dma((count,)),
        ]

    scratch = [
        vm((fc, width, fw), BF16),
        vm((fc, width, fw), BF16),
        vm((dc, hidden_w, dw), BF16),
        dma((2 * fc + dc,)),
        vm((ticks, tok, width), BF16),
        dma((ticks,)),
        dma((ticks,)),
        dma((2,)),
        dma((2,)),
    ] + landing(ticks)
    others = max(1, pairs - 1)
    for level in range(levels):
        count = ticks - level
        half = count * chips * tok
        scratch += [
            vm((count, tok, width), BF16),
            vm((count, tok, width + 128), BF16),
            vm((chips, pairs, count, tok, width + 128), BF16),
            dma((chips,)),
            dma((chips, others)),
            dma((chips, pairs)),
            vm((pairs * half, width), BF16),
            vm((fc, pairs * half, fw), BF16),
            vm((dc, pairs, half, dw), BF16),
            vm((dc, others, half, dw), BF16),
            dma((dc, others)),
            dma((dc, others)),
            vm((count, tok, 128), F32),
            dma((count, 2)),
            vm((count, dc, chips, tok, dw), BF16),
            dma((count, dc, chips)),
        ] + landing(count)
    scratch.append(vm((2, tok, width), BF16))
    sizes = (sections, chips, pairs, ticks, tok, width, hidden_w, fw, dw, levels)
    in_vmem = pl.BlockSpec(memory_space=pltpu.VMEM)
    anywhere = pl.BlockSpec(memory_space=pl.ANY)
    both = pl.pallas_call(
        functools.partial(window_kernel, sizes),
        out_shape=jax.ShapeDtypeStruct((2, tok, width), BF16),
        in_specs=[
            in_vmem,
            in_vmem,
            pl.BlockSpec(memory_space=pltpu.SMEM),
            in_vmem,
            in_vmem,
            anywhere,
            anywhere,
            anywhere,
        ],
        out_specs=in_vmem,
        scratch_shapes=scratch,
        compiler_params=pltpu.CompilerParams(
            collective_id=0, has_side_effects=True, vmem_limit_bytes=60 * 1024 * 1024
        ),
    )(act, queue, jnp.transpose(picks, (0, 2, 3, 1)), gain, jnp.swapaxes(table, 1, 2), gate_w, up_w, down_w)
    return both[0:1], both[1:2]


def solution(mesh):
    in_specs = (
        P("section", ("groups", "expert", "pair"), None),
        P("section", ("groups", "expert", "pair"), None),
        P("section", None, ("groups", "expert", "pair"), None),
        P("section", None),
        P("section", None, None),
        P("section", "pair", None, "expert"),
        P("section", "pair", None, "expert"),
        P("section", "pair", "expert", None),
    )
    out_specs = (
        P("section", ("groups", "expert", "pair"), None),
        P("section", ("groups", "expert", "pair"), None),
    )
    return jax.shard_map(body, mesh=mesh, in_specs=in_specs, out_specs=out_specs, check_vma=False)
```
